8 devices in a mesh: dp: 2 (over z, y), sp: 4 (over x, core).
Axes of the slice: x: 2, y: 2, z: 1, core: 2. Of those that a mesh axis runs over, the one named last changes fastest.
Arguments:
- x: bfloat16 [64, 256, 256], P('dp', 'sp'), parts along dimension 0
- w_cur: bfloat16 [16, 8, 256, 512], replicated
- w_past: bfloat16 [16, 8, 256, 512], replicated
- w_res: bfloat16 [16, 8, 256, 256], replicated
- w_skip: bfloat16 [16, 8, 256, 256], replicated
Outputs:
- output 1: float32 [64, 4, 64, 256], P('dp', 'sp'), parts along dimension 0
- output 2: float32 [64, 4, 64, 256], P('dp', 'sp'), parts along dimension 0
There are 2 independent parts. The reference program is written for one: setup_inputs(seed, part) draws one part's arguments, and reference() takes and returns one part's arrays. A program takes and returns all parts, laid end to end along the dimension named above; an argument that names none is the same for every part.
All inputs are finite; a program needn't handle non-finite values.
Results may differ from the reference program's by a relative error of at most 0.00873732.
Values are sent between devices in bfloat16 or wider.
A program may use at most 1 GiB of HBM per device.

```python
import jax
import jax.numpy as jnp
from jax import lax

BATCH_PART = 32
SEQ_DEV = 64
GROUP_SIZE = 4
STACKS = 16
CHANNELS = 256
SKIP_CH = 256
CYCLE_LEN = 8

SEQ_LEN = SEQ_DEV * GROUP_SIZE
LAYERS = STACKS * CYCLE_LEN


def setup_inputs(seed: int = 0, part: int = 0) -> dict:
    base_key = jax.random.key(seed)
    key_x = jax.random.fold_in(jax.random.fold_in(base_key, 1), part)
    key_w = jax.random.split(jax.random.fold_in(base_key, 2), 4)
    tap_scale = (2 * CHANNELS) ** -0.5
    out_scale = 2.0 * (CHANNELS * LAYERS) ** -0.5
    tap_shape = (STACKS, CYCLE_LEN, CHANNELS, 2 * CHANNELS)
    x = jax.random.normal(key_x, (BATCH_PART, SEQ_LEN, CHANNELS), jnp.float32)
    w_cur = jax.random.normal(key_w[0], tap_shape, jnp.float32) * tap_scale
    w_past = jax.random.normal(key_w[1], tap_shape, jnp.float32) * tap_scale
    w_res = jax.random.normal(key_w[2], (STACKS, CYCLE_LEN, CHANNELS, CHANNELS), jnp.float32) * out_scale
    w_skip = jax.random.normal(key_w[3], (STACKS, CYCLE_LEN, CHANNELS, SKIP_CH), jnp.float32) * out_scale
    return {"x": x.astype(jnp.bfloat16), "w_cur": w_cur.astype(jnp.bfloat16), "w_past": w_past.astype(jnp.bfloat16), "w_res": w_res.astype(jnp.bfloat16), "w_skip": w_skip.astype(jnp.bfloat16)}


def gated_layer(h_res, skip_acc, cur_w, past_w, res_w, skip_w, dilation):
    row_count = BATCH_PART * SEQ_LEN
    u_cur = h_res.astype(jnp.bfloat16)
    u_past = jnp.concatenate([jnp.zeros((BATCH_PART, dilation, CHANNELS), jnp.bfloat16), u_cur[:, :SEQ_LEN - dilation]], axis=1)
    pre_act = jnp.dot(u_cur.reshape(row_count, CHANNELS), cur_w, preferred_element_type=jnp.float32) + jnp.dot(u_past.reshape(row_count, CHANNELS), past_w, preferred_element_type=jnp.float32)
    gated = (jnp.tanh(pre_act[:, :CHANNELS]) * jax.nn.sigmoid(pre_act[:, CHANNELS:])).astype(jnp.bfloat16)
    h_new = h_res + jnp.dot(gated, res_w, preferred_element_type=jnp.float32).reshape(BATCH_PART, SEQ_LEN, CHANNELS)
    skip_new = skip_acc + jnp.dot(gated, skip_w, preferred_element_type=jnp.float32).reshape(BATCH_PART, SEQ_LEN, SKIP_CH)
    return h_new, skip_new


def reference(x, w_cur, w_past, w_res, w_skip):
    def stack_body(carry, weights):
        h_res, skip_acc = carry
        stack_cur, stack_past, stack_res, stack_skip = weights
        for layer_pos in range(CYCLE_LEN):
            h_res, skip_acc = gated_layer(h_res, skip_acc, stack_cur[layer_pos], stack_past[layer_pos], stack_res[layer_pos], stack_skip[layer_pos], 2 ** layer_pos)
        return (h_res, skip_acc), None

    h_start = x.astype(jnp.float32)
    skip_start = jnp.zeros((BATCH_PART, SEQ_LEN, SKIP_CH), jnp.float32)
    (h_fin, skip_fin), unused = lax.scan(stack_body, (h_start, skip_start), (w_cur, w_past, w_res, w_skip))
    h_out = h_fin.reshape(BATCH_PART, SEQ_DEV, GROUP_SIZE, CHANNELS).transpose(0, 2, 1, 3)
    skip_out = skip_fin.reshape(BATCH_PART, SEQ_DEV, GROUP_SIZE, SKIP_CH).transpose(0, 2, 1, 3)
    return (h_out, skip_out)
```

```python
import jax
import jax.numpy as jnp
from jax import lax
from jax.experimental import pallas as pl
from jax.experimental.pallas import tpu as pltpu
from jax.sharding import PartitionSpec as P

F32, BF16 = jnp.float32, jnp.bfloat16

HEAD = 1
TAIL = 4
SLOTS = TAIL + 1
M_WIDE = 512
M_BLK = 128
LAG_WIDE = 1
LAG_BLK = 1


def solution(mesh):
    G = mesh.shape["sp"]

    def kernel(x, wc, wp, wr, ws, ho, so, h, sk, u, bc, bp, br, bs, b1, b2, b3, b4, b5, b6, b7, e8, xb, st, wsem, xsend, xrecv, xloc, osend, orecv, oloc):
        batch, seq_blk, C = x.shape
        S, L = wc.shape[0], wc.shape[1]
        NB = batch // G
        RB = seq_blk * NB
        R = RB * G
        PAD = u.shape[1] - R
        OL = seq_blk // G
        me = lax.axis_index("sp")
        hist = {1: b1, 2: b2, 3: b3, 4: b4, 5: b5, 6: b6, 7: b7}

        def rows(ref, r, m, stride=None):
            return jnp.concatenate([ref[k, pl.ds(r, m, stride=stride), :] for k in range(2)], axis=1)

        def put(ref, r, m, v, stride=None):
            for k in range(2):
                ref[k, pl.ds(r, m, stride=stride), :] = v[:, k * C // 2:(k + 1) * C // 2]

        def weights(s, slot):
            pairs = ((wc, bc), (wp, bp), (wr, br), (ws, bs))
            return [pltpu.make_async_copy(src.at[s], dst.at[slot], wsem.at[slot, k]) for k, (src, dst) in enumerate(pairs)]

        def start_weights(s):
            for c in weights(s, lax.rem(s, SLOTS)):
                c.start()

        def wait_weights(s):
            for c in weights(s, lax.rem(s, SLOTS)):
                c.wait()

        def x_remote(o, src):
            peer = lax.rem(me + o, G)
            return pltpu.make_async_remote_copy(
                src_ref=x.at[pl.ds(peer * NB, NB)], dst_ref=xb.at[src], send_sem=xsend.at[o], recv_sem=xrecv.at[src],
                device_id={"sp": peer}, device_id_type=pl.DeviceIdType.MESH)

        def x_local():
            return pltpu.make_async_copy(x.at[pl.ds(me * NB, NB)], xb.at[me], xloc)

        def out_remote(b, q, o, src):
            peer = lax.rem(me + o, G)
            dst = (ho, so)[q]
            return pltpu.make_async_remote_copy(
                src_ref=st.at[b, q, peer], dst_ref=dst.at[pl.ds(src * NB, NB), 0, pl.ds(OL * b, OL), :],
                send_sem=osend.at[b, q, o], recv_sem=orecv.at[b, q, src],
                device_id={"sp": peer}, device_id_type=pl.DeviceIdType.MESH)

        def out_local(b, q):
            dst = (ho, so)[q]
            return pltpu.make_async_copy(st.at[b, q, me], dst.at[pl.ds(me * NB, NB), 0, pl.ds(OL * b, OL), :], oloc.at[b, q])

        for s in range(SLOTS):
            start_weights(s)
        barrier = pltpu.get_barrier_semaphore()
        for o in range(1, G):
            pl.semaphore_signal(barrier, inc=1, device_id={"sp": lax.rem(me + o, G)}, device_id_type=pl.DeviceIdType.MESH)
        x_local().start()
        pl.semaphore_wait(barrier, G - 1)
        for o in range(1, G):
            x_remote(o, me).start()

        u[:, pl.ds(0, PAD), :] = jnp.zeros((2, PAD, C), BF16)
        put(h, 0, NB, jnp.zeros((NB, C), F32))

        def load_block(b):
            @pl.when(me == b)
            def _():
                x_local().wait()

            @pl.when(me != b)
            def _():
                x_remote(1, b).wait_recv()

            for bb in range(NB):
                put(h, NB + RB * b + bb, seq_blk, xb[b, bb].astype(F32), stride=NB)
            u[0, pl.ds(PAD + RB * b, RB), :] = rows(h, NB + RB * b, RB).astype(BF16)
            put(sk, RB * b, RB, jnp.zeros((RB, C), F32))

        def send_block(b):
            for q in range(2):
                src, base = ((h, NB), (sk, 0))[q]
                for j in range(G):
                    for bb in range(NB):
                        st[b, q, j, bb] = rows(src, base + RB * b + NB * j + bb, OL, stride=NB * G)
            for o in range(1, G):
                for q in range(2):
                    out_remote(b, q, o, me).start()
            for q in range(2):
                out_local(b, q).start()

        def pipeline(tasks, lag, g1, g2):
            zs = {}
            for k in range(len(tasks) + lag):
                if k < len(tasks):
                    zs[tasks[k]] = g1(*tasks[k])
                if k >= lag:
                    g2(*tasks[k - lag], zs.pop(tasks[k - lag]))

        def preact(cur, past, slot, i):
            z = jnp.dot(cur, bc[slot, i], preferred_element_type=F32)
            if past is not None:
                z = z + jnp.dot(past, bp[slot, i], preferred_element_type=F32)
            return z

        def update(z, slot, i, r0, m):
            a = (jnp.tanh(z[:, :C]) * jax.nn.sigmoid(z[:, C:])).astype(BF16)
            hn = rows(h, NB + r0, m) + jnp.dot(a, br[slot, i], preferred_element_type=F32)
            put(h, NB + r0, m, hn)
            put(sk, r0, m, rows(sk, r0, m) + jnp.dot(a, bs[slot, i], preferred_element_type=F32))
            return hn.astype(BF16)

        def wide_stack(s, carry):
            slot = lax.rem(s, SLOTS)
            wait_weights(s)

            @pl.when(s == HEAD)
            def _():
                for k in range(HEAD):
                    start_weights(k + SLOTS)

            @pl.when((s > HEAD) & (s - 1 + SLOTS < S))
            def _():
                start_weights(s - 1 + SLOTS)

            def g1(i, c):
                off, r0 = NB << i, c * M_WIDE
                past = None
                if r0 + M_WIDE > off:
                    if i == 0:
                        past = rows(h, NB + r0 - off, M_WIDE).astype(BF16)
                    else:
                        past = u[i % 2, pl.ds(PAD + r0 - off, M_WIDE), :]
                return preact(u[i % 2, pl.ds(PAD + r0, M_WIDE), :], past, slot, i)

            def g2(i, c, z):
                r0 = c * M_WIDE
                u[(i + 1) % 2, pl.ds(PAD + r0, M_WIDE), :] = update(z, slot, i, r0, M_WIDE)

            pipeline([(i, c) for i in range(L) for c in range(R // M_WIDE)], LAG_WIDE, g1, g2)
            return carry

        def block_stack(b, s, k):
            slot = lax.rem(s, SLOTS)
            if b == 0:
                wait_weights(s)
            last = RB // M_BLK - 1

            def place(i):
                off = NB << i
                return off if off < RB else RB * b

            def g1(i, c):
                off, r0 = NB << i, RB * b + c * M_BLK
                past = None
                if i == 0:
                    cur = u[0, pl.ds(PAD + r0, M_BLK), :]
                    if c == 0:
                        first = jnp.zeros((NB, C), F32) if b == 0 else e8[k]
                        past = jnp.concatenate([first, rows(h, NB + r0, M_BLK - NB)], axis=0).astype(BF16)
                    else:
                        past = rows(h, r0, M_BLK).astype(BF16)
                    if c == last and b < G - 1:
                        e8[k] = rows(h, r0 + M_BLK, NB)
                else:
                    buf = hist[i]
                    cur = buf[k, pl.ds(place(i) + c * M_BLK, M_BLK), :]
                    if b == 0 and c == 0 and off < RB:
                        buf[k, pl.ds(0, off), :] = jnp.zeros((off, C), BF16)
                    if r0 + M_BLK > off:
                        past = buf[k, pl.ds(place(i) + c * M_BLK - off, M_BLK), :]
                    if c == last and b < G - 1 and off < RB:
                        buf[k, pl.ds(0, off), :] = buf[k, pl.ds(RB, off), :]
                return preact(cur, past, slot, i)

            def g2(i, c, z):
                r0 = RB * b + c * M_BLK
                un = update(z, slot, i, r0, M_BLK)
                if i == L - 1:
                    u[0, pl.ds(PAD + r0, M_BLK), :] = un
                else:
                    hist[i + 1][k, pl.ds(place(i + 1) + c * M_BLK, M_BLK), :] = un

            pipeline([(i, c) for i in range(L) for c in range(last + 1)], LAG_BLK, g1, g2)

        def phase(p, carry):
            lo = p * (S - TAIL)
            n = jnp.where(p == 0, HEAD, TAIL)
            for b in range(G):
                @pl.when(p == 0)
                def _():
                    load_block(b)

                def step(k, carry):
                    block_stack(b, lo + k, k)
                    return carry

                lax.fori_loop(0, n, step, 0)

                @pl.when(p == 1)
                def _():
                    send_block(b)

            lax.fori_loop(HEAD, jnp.where(p == 0, S - TAIL, HEAD), wide_stack, 0)
            return carry

        lax.fori_loop(0, 2, phase, 0)

        for o in range(1, G):
            x_remote(o, me).wait_send()
        for b in range(G):
            for q in range(2):
                out_local(b, q).wait()
                for o in range(1, G):
                    out_remote(b, q, o, me).wait_send()
                    out_remote(b, q, o, lax.rem(me + G - o, G)).wait_recv()

    def local(x, wc, wp, wr, ws):
        batch, seq_blk, C = x.shape
        S, L = wc.shape[0], wc.shape[1]
        NB = batch // G
        RB = seq_blk * NB
        R = RB * G
        KB = max(HEAD, TAIL)
        hist = [pltpu.VMEM((KB, (NB << i) + RB if (NB << i) < RB else R, C), BF16) for i in range(1, L)]
        hbm = pl.BlockSpec(memory_space=pltpu.HBM)
        out = jax.ShapeDtypeStruct((batch, 1, seq_blk, C), F32)
        return pl.pallas_call(
            kernel,
            out_shape=[out, out],
            in_specs=[hbm] * 5,
            out_specs=[hbm] * 2,
            scratch_shapes=[
                pltpu.VMEM((2, R + NB, C // 2), F32),
                pltpu.VMEM((2, R, C // 2), F32),
                pltpu.VMEM((2, R + M_WIDE // 2, C), BF16),
                pltpu.VMEM((SLOTS, L, C, 2 * C), BF16),
                pltpu.VMEM((SLOTS, L, C, 2 * C), BF16),
                pltpu.VMEM((SLOTS, L, C, C), BF16),
                pltpu.VMEM((SLOTS, L, C, C), BF16),
                *hist,
                pltpu.VMEM((KB, NB, C), F32),
                pltpu.VMEM((G, NB, seq_blk, C), BF16),
                pltpu.VMEM((G, 2, G, NB, seq_blk // G, C), F32),
                pltpu.SemaphoreType.DMA((SLOTS, 4)),
                pltpu.SemaphoreType.DMA((G,)),
                pltpu.SemaphoreType.DMA((G,)),
                pltpu.SemaphoreType.DMA,
                pltpu.SemaphoreType.DMA((G, 2, G)),
                pltpu.SemaphoreType.DMA((G, 2, G)),
                pltpu.SemaphoreType.DMA((G, 2)),
            ],
            compiler_params=pltpu.CompilerParams(collective_id=0, has_side_effects=True, vmem_limit_bytes=67000000),
            name="stack",
        )(x, wc, wp, wr, ws)

    return jax.shard_map(local, mesh=mesh, in_specs=(P("dp", "sp", None), P(), P(), P(), P()), out_specs=(P("dp", "sp", None, None), P("dp", "sp", None, None)), check_vma=False)
```

```python
import jax
import jax.numpy as jnp
from jax import lax
from jax.experimental import pallas as pl
from jax.experimental.pallas import tpu as pltpu
from jax.sharding import PartitionSpec as P

F32, BF16 = jnp.float32, jnp.bfloat16

TAIL = 3
SLOTS = 4
M_WIDE = 512
M_BLK = 128
VMEM = 48 << 20


def solution(mesh):
    G = mesh.shape["sp"]

    def kernel(x, wc, wp, wr, ws, ho, so, h, sk, u, bc, bp, br, bs, b1, b2, b3, b4, b5, b6, b7, e8, hb, skb, ub, xb, st, wsem, xsend, xrecv, xloc, osend, orecv, oloc):
        batch, seq_blk, C = x.shape
        S, L = wc.shape[0], wc.shape[1]
        NB = batch // G
        RB = seq_blk * NB
        R = RB * G
        PAD = u.shape[1] - R
        OL = seq_blk // G
        me = lax.axis_index("sp")
        hist = {1: b1, 2: b2, 3: b3, 4: b4, 5: b5, 6: b6, 7: b7}

        def rows(ref, r, m, stride=None):
            return jnp.concatenate([ref[k, pl.ds(r, m, stride=stride), :] for k in range(2)], axis=1)

        def put(ref, r, m, v, stride=None):
            for k in range(2):
                ref[k, pl.ds(r, m, stride=stride), :] = v[:, k * C // 2:(k + 1) * C // 2]

        def weights(s, slot):
            pairs = ((wc, bc), (wp, bp), (wr, br), (ws, bs))
            return [pltpu.make_async_copy(src.at[s], dst.at[slot], wsem.at[slot, k]) for k, (src, dst) in enumerate(pairs)]

        def start_weights(s):
            for c in weights(s, lax.rem(s, SLOTS)):
                c.start()

        def wait_weights(s):
            for c in weights(s, lax.rem(s, SLOTS)):
                c.wait()

        def x_remote(o, src):
            peer = lax.rem(me + o, G)
            return pltpu.make_async_remote_copy(
                src_ref=x.at[pl.ds(peer * NB, NB)], dst_ref=xb.at[src], send_sem=xsend.at[o], recv_sem=xrecv.at[src],
                device_id={"sp": peer}, device_id_type=pl.DeviceIdType.MESH)

        def x_local():
            return pltpu.make_async_copy(x.at[pl.ds(me * NB, NB)], xb.at[me], xloc)

        def out_remote(b, q, o, src):
            peer = lax.rem(me + o, G)
            dst = (ho, so)[q]
            return pltpu.make_async_remote_copy(
                src_ref=st.at[lax.rem(b, 2), q, peer], dst_ref=dst.at[pl.ds(src * NB, NB), 0, pl.ds(OL * b, OL), :],
                send_sem=osend.at[b, q, o], recv_sem=orecv.at[b, q, src],
                device_id={"sp": peer}, device_id_type=pl.DeviceIdType.MESH)

        def out_local(b, q):
            dst = (ho, so)[q]
            return pltpu.make_async_copy(st.at[lax.rem(b, 2), q, me], dst.at[pl.ds(me * NB, NB), 0, pl.ds(OL * b, OL), :], oloc.at[b, q])

        for s in range(1):
            start_weights(s)
        barrier = pltpu.get_barrier_semaphore()
        for o in range(1, G):
            pl.semaphore_signal(barrier, inc=1, device_id={"sp": lax.rem(me + o, G)}, device_id_type=pl.DeviceIdType.MESH)
        x_local().start()
        pl.semaphore_wait(barrier, G - 1)
        odd = lax.rem(me, 2) == 1
        x_near = [lax.rem(me, 2) * (G - 2) + 1, G // 2, G - 1 - lax.rem(me, 2) * (G - 2)]

        def send_x_far():
            x_remote(x_near[1], me).start()
            x_remote(x_near[2], me).start()

        @pl.when(jnp.logical_not(odd))
        def _():
            send_x_far()

        x_remote(x_near[0], me).start()

        u[:, pl.ds(0, PAD), :] = jnp.zeros((2, PAD, C), BF16)
        put(h, 0, NB, jnp.zeros((NB, C), F32))

        def load_block(b):
            @pl.when(me == b)
            def _():
                x_local().wait()

            @pl.when(me != b)
            def _():
                x_remote(1, b).wait_recv()

            for bb in range(NB):
                put(hb, bb, seq_blk, xb[b, bb].astype(F32), stride=NB)
            ub[...] = rows(hb, 0, RB).astype(BF16)
            skb[...] = jnp.zeros_like(skb)

        def block_views(b):
            r0 = pl.multiple_of(RB * b, RB)
            return ((hb, h.at[:, pl.ds(pl.multiple_of(r0 + NB, NB), RB), :]), (skb, sk.at[:, pl.ds(r0, RB), :]),
                    (ub, u.at[0, pl.ds(pl.multiple_of(PAD + r0, M_BLK), RB), :]))

        def fetch_block(b):
            for small, full in block_views(b):
                small[...] = full[...]

        def store_block(b):
            for small, full in block_views(b):
                full[...] = small[...]

        def sent(b):
            for q in range(2):
                out_local(b, q).wait()
                for o in range(1, G):
                    out_remote(b, q, o, me).wait_send()

        def send_block(b):
            @pl.when(b >= 2)
            def _():
                sent(b - 2)

            for q in range(2):
                src = (hb, skb)[q]
                for j in range(G):
                    for bb in range(NB):
                        st[lax.rem(b, 2), q, j, bb] = rows(src, NB * j + bb, OL, stride=NB * G)
            for o in range(1, G):
                for q in range(2):
                    out_remote(b, q, o, me).start()
            for q in range(2):
                out_local(b, q).start()

        def wide_order(n):
            tasks = [(i, c) for i in range(L) for c in range(n)]
            for prev, cur in zip([None] + tasks, tasks + [None]):
                if cur:
                    yield 1, *cur
                if prev:
                    yield 2, *prev

        def block_order(n):
            for i in range(n):
                yield 1, i, 0
                if i:
                    yield 2, i - 1, 3
                for half, c in ((1, 1), (1, 2), (2, 0), (1, 3), (2, 1), (2, 2)):
                    yield half, i, c
            yield 2, n - 1, 3

        def pipeline(order, g1, g2):
            zs = {}
            for half, i, c in order:
                if half == 1:
                    zs[i, c] = g1(i, c)
                else:
                    g2(i, c, zs.pop((i, c)))

        def preact(cur, past, slot, i):
            z = jnp.dot(cur, bc[slot, i], preferred_element_type=F32)
            if past is not None:
                z = z + jnp.dot(past, bp[slot, i], preferred_element_type=F32)
            return z

        def update(z, slot, i, r0, m, h=h, sk=sk, pad=None):
            pad = NB if pad is None else pad
            a = (jnp.tanh(z[:, :C]) * jax.nn.sigmoid(z[:, C:])).astype(BF16)
            hn = rows(h, r0 + pad, m) + jnp.dot(a, br[slot, i], preferred_element_type=F32)
            put(h, r0 + pad, m, hn)
            put(sk, r0, m, rows(sk, r0, m) + jnp.dot(a, bs[slot, i], preferred_element_type=F32))
            return hn.astype(BF16)

        def wide_stack(s, carry):
            slot = lax.rem(s, SLOTS)
            wait_weights(s)

            @pl.when(s - 1 + SLOTS < S)
            def _():
                start_weights(s - 1 + SLOTS)

            def g1(i, c):
                off, r0 = NB << i, c * M_WIDE
                past = None
                if r0 + M_WIDE > off:
                    if i == 0:
                        past = rows(h, NB + r0 - off, M_WIDE).astype(BF16)
                    else:
                        past = u[i % 2, pl.ds(PAD + r0 - off, M_WIDE), :]
                return preact(u[i % 2, pl.ds(PAD + r0, M_WIDE), :], past, slot, i)

            def g2(i, c, z):
                r0 = c * M_WIDE
                u[(i + 1) % 2, pl.ds(PAD + r0, M_WIDE), :] = update(z, slot, i, r0, M_WIDE)

            pipeline(wide_order(R // M_WIDE), g1, g2)
            return carry

        def clear_history():
            e8[...] = jnp.zeros_like(e8)
            for i, buf in hist.items():
                for k in range(TAIL):
                    buf[k, pl.ds(0, NB << i), :] = jnp.zeros((NB << i, C), BF16)

        def block_stacks(s0, count):
            last = RB // M_BLK - 1

            def g1(n, c):
                k, i = n // L, n % L
                slot, off, r0 = lax.rem(s0 + k, SLOTS), NB << i, c * M_BLK
                if i == 0:
                    cur = ub[pl.ds(r0, M_BLK), :]
                    if c == 0:
                        past = jnp.concatenate([e8[k], rows(hb, 0, M_BLK - NB)], axis=0).astype(BF16)
                    else:
                        past = rows(hb, r0 - NB, M_BLK).astype(BF16)
                    if c == last:
                        e8[k] = rows(hb, RB - NB, NB)
                else:
                    buf = hist[i]
                    cur = buf[k, pl.ds(off + r0, M_BLK), :]
                    past = buf[k, pl.ds(r0, M_BLK), :]
                    if c == last:
                        for r in range(0, off, RB):
                            n_rows = min(off, RB)
                            buf[k, pl.ds(r, n_rows), :] = buf[k, pl.ds(r + RB, n_rows), :]
                return preact(cur, past, slot, i)

            def g2(n, c, z):
                k, i = n // L, n % L
                un = update(z, lax.rem(s0 + k, SLOTS), i, c * M_BLK, M_BLK, hb, skb, 0)
                if i == L - 1:
                    ub[pl.ds(c * M_BLK, M_BLK), :] = un
                else:
                    hist[i + 1][k, pl.ds((NB << (i + 1)) + c * M_BLK, M_BLK), :] = un

            pipeline(block_order(count * L), g1, g2)

        def head(b, carry):
            load_block(b)
            block_stacks(0, 1)
            store_block(b)

            @pl.when((b == 0) & odd)
            def _():
                send_x_far()

            return carry

        def tail(b, carry):
            fetch_block(b)
            block_stacks(S - TAIL, TAIL)
            send_block(b)
            return carry

        clear_history()
        wait_weights(0)
        for s in range(1, SLOTS):
            start_weights(s)
        lax.fori_loop(0, G, head, 0)
        lax.fori_loop(1, S - TAIL, wide_stack, 0)
        clear_history()
        for k in range(TAIL):
            wait_weights(S - TAIL + k)
        lax.fori_loop(0, G, tail, 0)

        for o in range(1, G):
            x_remote(o, me).wait_send()
        for b in range(G - 2, G):
            sent(b)
        for b in range(G):
            for q in range(2):
                for o in range(1, G):
                    out_remote(b, q, o, lax.rem(me + G - o, G)).wait_recv()

    def local(x, wc, wp, wr, ws):
        batch, seq_blk, C = x.shape
        S, L = wc.shape[0], wc.shape[1]
        NB = batch // G
        RB = seq_blk * NB
        R = RB * G
        hist = [pltpu.VMEM((TAIL, (NB << i) + RB, C), BF16) for i in range(1, L)]
        hbm = pl.BlockSpec(memory_space=pltpu.HBM)
        out = jax.ShapeDtypeStruct((batch, 1, seq_blk, C), F32)
        return pl.pallas_call(
            kernel,
            out_shape=[out, out],
            in_specs=[hbm] * 5,
            out_specs=[pl.BlockSpec(memory_space=pl.ANY)] * 2,
            scratch_shapes=[
                pltpu.VMEM((2, R + NB, C // 2), F32),
                pltpu.VMEM((2, R, C // 2), F32),
                pltpu.VMEM((2, R + M_WIDE // 2, C), BF16),
                pltpu.VMEM((SLOTS, L, C, 2 * C), BF16),
                pltpu.VMEM((SLOTS, L, C, 2 * C), BF16),
                pltpu.VMEM((SLOTS, L, C, C), BF16),
                pltpu.VMEM((SLOTS, L, C, C), BF16),
                *hist,
                pltpu.VMEM((TAIL, NB, C), F32),
                pltpu.VMEM((2, RB, C // 2), F32),
                pltpu.VMEM((2, RB, C // 2), F32),
                pltpu.VMEM((RB, C), BF16),
                pltpu.VMEM((G, NB, seq_blk, C), BF16),
                pltpu.VMEM((2, 2, G, NB, seq_blk // G, C), F32),
                pltpu.SemaphoreType.DMA((SLOTS, 4)),
                pltpu.SemaphoreType.DMA((G,)),
                pltpu.SemaphoreType.DMA((G,)),
                pltpu.SemaphoreType.DMA,
                pltpu.SemaphoreType.DMA((G, 2, G)),
                pltpu.SemaphoreType.DMA((G, 2, G)),
                pltpu.SemaphoreType.DMA((G, 2)),
            ],
            compiler_params=pltpu.CompilerParams(collective_id=0, has_side_effects=True, vmem_limit_bytes=VMEM),
            name="stack",
        )(x, wc, wp, wr, ws)

    return jax.shard_map(local, mesh=mesh, in_specs=(P("dp", "sp", None), P(), P(), P(), P()), out_specs=(P("dp", "sp", None, None), P("dp", "sp", None, None)), check_vma=False)
```
